32 devices in a mesh: wide: 4 (over y, x), narrow: 8 (over z, core).
Axes of the slice: x: 2, y: 2, z: 4, core: 2. Of those that a mesh axis runs over, the one named last changes fastest.
Arguments:
- tokens: bfloat16 [4096, 4096], P('narrow'), may hold values from -6 to 6
- norm_gain: float32 [4096], replicated, may hold values from 0.1 to 1.9
- coded: bfloat16 [4096, 14336], P('narrow', 'wide'), may hold values from -0.09375 to 0.09375
- block_codes: int32 [32, 112], P('narrow', 'wide'), may hold values from 0 to 15
- grid: float32 [16], replicated, may hold values from 0.5 to 2
- cotangent: bfloat16 [4096, 14336], P('narrow', 'wide'), may hold values from -6 to 6
Outputs:
- activated: bfloat16 [4096, 14336], P('narrow', 'wide')
- weight_grad: float32 [4096, 14336], P('narrow', 'wide')
- input_grad: bfloat16 [4096, 4096], P('narrow', 'wide')
The draws below stay inside these ranges and needn't reach their ends.
All inputs are finite; a program needn't handle non-finite values.
Results may differ from the reference program's by a relative error of at most 0.017.
Values may be sent and summed in bfloat16 or wider, within the bound.
No kernel may reach another device: no remote copies, remote signals or barrier semaphores. Data moves between devices by JAX's collectives and lax.ppermute only.
A program may use at most 128 MiB of HBM per device.

```python
import math
import jax
import jax.numpy as jnp
from jax import lax

D = 4096
FFW = 14336
BLOCK = 128
LEVELS = 16
TOK_DEV = 512
TOKENS = 4096
N_WIDE = 4
N_NARROW = 8


def place_ends(result, rng, low, high):
    extent = result.shape
    index_at = [jax.random.randint(jax.random.fold_in(rng, axis), (), 0, extent[axis]) for axis in range(len(extent))]
    result = result.at[tuple(index_at)].set(low)
    longest = extent.index(max(extent))
    index_at[longest] = (index_at[longest] + 1) % extent[longest]
    return result.at[tuple(index_at)].set(high)


def shard_levels(key, dims, pieces, low, top_value):
    def one(axis_at, blocks):
        heights = jax.random.uniform(jax.random.fold_in(jax.random.fold_in(key, 6), axis_at), (blocks,), jnp.float32, low / len(pieces), top_value / len(pieces))
        return jnp.repeat(jnp.exp(heights), dims[axis_at] // blocks).reshape((-1,) + (1,) * (len(dims) - axis_at - 1))

    loudness = one(*pieces[0])
    for cut in pieces[1:]:
        loudness = loudness * one(*cut)
    return loudness


def bell_draw(stream_key, extent, scale, most, cuts=(), held_as=jnp.bfloat16):
    factor_of = shard_levels(stream_key, extent, cuts, -0.22, 0.18) if cuts else 1.0
    values = jax.random.normal(stream_key, extent, jnp.float32) * scale * factor_of
    return jnp.minimum(jnp.maximum(values, -most), most).astype(held_as)


def setup_inputs(seed: int = 0) -> dict:
    seeds = jax.random.split(jax.random.key(seed), 7)
    return {
        "tokens": bell_draw(seeds[0], (TOKENS, D), 1.0, 6.0, ((0, 8),)),
        "norm_gain": jnp.clip(1.0 + 0.18 * jax.random.normal(seeds[1], (D,), jnp.float32), 0.1, 1.9),
        "coded": bell_draw(seeds[2], (D, FFW), D ** -0.5, 0.09375, ((0, 8), (1, 4))),
        "block_codes": place_ends(jax.random.randint(seeds[3], (D // BLOCK, FFW // BLOCK), 0, LEVELS), jax.random.fold_in(seeds[3], 1), 0, LEVELS - 1).astype(jnp.int32),
        "grid": jnp.clip(jnp.exp(jax.random.uniform(seeds[4], (LEVELS,), jnp.float32, math.log(0.5), math.log(2.0))), 0.5, 2.0),
        "cotangent": bell_draw(seeds[5], (TOKENS, FFW), 1.0, 6.0, ((0, 8), (1, 4))),
    }


def hadamard(size):
    index = jnp.arange(size, dtype=jnp.int32)
    parity = jnp.zeros((size, size), jnp.int32)
    for level in range(size.bit_length() - 1):
        stride = 2 ** level
        parity = parity + index[:, None] // stride % 2 * (index[None, :] // stride % 2)
    return (1 - 2 * (parity % 2)).astype(jnp.bfloat16)

def decode(coded, block_codes, grid):
    nrows, ncols = coded.shape
    rotation = hadamard(BLOCK).astype(jnp.float32)
    onehot = (block_codes[:, :, None] == jnp.arange(grid.shape[0], dtype=jnp.int32)[None, None, :]).astype(jnp.float32)
    block_scale = lax.optimization_barrier(jnp.sum(onehot * grid[None, None, :], axis=-1)) / jnp.sqrt(jnp.float32(BLOCK))
    blocks = coded.reshape(nrows // BLOCK, BLOCK, ncols // BLOCK, BLOCK)

    def one_row(pair):
        piece, scales = pair
        turned = jnp.einsum('ikj,jl->ikl', piece.astype(jnp.float32), rotation)
        return (turned * scales[None, :, None]).reshape(BLOCK, ncols).astype(jnp.bfloat16)
    return lax.map(one_row, (blocks, block_scale)).reshape(nrows, ncols)

def reference(tokens, norm_gain, coded, block_codes, grid, cotangent):
    weight = decode(coded, block_codes, grid)
    inputs = tokens.astype(jnp.float32)
    inv_rms = lax.rsqrt(lax.optimization_barrier(jnp.mean(inputs * inputs, axis=-1, keepdims=True)) + 1e-05)
    normed = (inputs * inv_rms * norm_gain[None, :]).astype(jnp.bfloat16)
    preact = jnp.dot(normed, weight, preferred_element_type=jnp.float32)
    sig = jax.nn.sigmoid(preact)
    activated = (preact * sig).astype(jnp.bfloat16)
    pre_grad = (cotangent.astype(jnp.float32) * sig * (1.0 + preact * (1.0 - sig))).astype(jnp.bfloat16)

    def add_group(group, total):
        rows_n = lax.dynamic_slice_in_dim(normed, group * TOK_DEV, TOK_DEV, 0)
        rows_g = lax.dynamic_slice_in_dim(pre_grad, group * TOK_DEV, TOK_DEV, 0)
        term = jnp.dot(rows_n.T, rows_g, preferred_element_type=jnp.float32)
        return total + term.astype(jnp.bfloat16).astype(jnp.float32)
    weight_grad = lax.fori_loop(0, N_NARROW, add_group, jnp.zeros((D, FFW), jnp.float32))
    width = FFW // N_WIDE

    def add_columns(group, total):
        cols_g = lax.dynamic_slice_in_dim(pre_grad, group * width, width, 1)
        cols_w = lax.dynamic_slice_in_dim(weight, group * width, width, 1)
        term = lax.dot_general(cols_g, cols_w, (((1,), (1,)), ((), ())), preferred_element_type=jnp.float32)
        return total + term.astype(jnp.bfloat16).astype(jnp.float32)
    normed_grad = lax.fori_loop(0, N_WIDE, add_columns, jnp.zeros((TOKENS, D), jnp.float32))
    scaled_grad = normed_grad * norm_gain[None, :]
    row_dot = lax.optimization_barrier(jnp.mean(scaled_grad * inputs, axis=-1, keepdims=True))
    input_grad = (inv_rms * scaled_grad - inputs * inv_rms ** 3 * row_dot).astype(jnp.bfloat16)
    return (activated, weight_grad, input_grad)
```

```python
import jax
import jax.numpy as jnp
from jax import lax
from jax.sharding import PartitionSpec as P


BLOCK = 128
CHUNKS = 4
DEPTH = 2


def hadamard(size):
    index = jnp.arange(size, dtype=jnp.int32)
    parity = jnp.zeros((size, size), jnp.int32)
    for level in range(size.bit_length() - 1):
        stride = 2**level
        parity = parity + index[:, None] // stride % 2 * (index[None, :] // stride % 2)
    return (1 - 2 * (parity % 2)).astype(jnp.bfloat16)


def turn(ncols):
    nblk = ncols // BLOCK
    tiled = jnp.tile(hadamard(BLOCK), (nblk, nblk))
    where = jnp.arange(ncols, dtype=jnp.int32) // BLOCK
    return jnp.where(where[:, None] == where[None, :], tiled, jnp.zeros_like(tiled))


def decode(coded, scale):
    _, cols = coded.shape
    turned = jnp.dot(coded, turn(cols), preferred_element_type=jnp.float32)
    wide_scale = jnp.repeat(jnp.repeat(scale, BLOCK, axis=0), BLOCK, axis=1)
    return (turned * wide_scale).astype(jnp.bfloat16)


def cuts(blocks, pieces):
    pieces = min(pieces, blocks)
    edges = [(blocks * i + pieces - 1) // pieces for i in range(pieces + 1)]
    return [(lo * BLOCK, hi * BLOCK) for lo, hi in zip(edges, edges[1:])]


def plan(n):
    out = [("share", 0), ("weight", 0), ("norm", 0), ("near", 0), ("far", 0)]
    out += [("weight", k) for k in range(1, min(DEPTH, n))]
    out += [("cot", 0), ("cross", 0)]
    for k in range(n):
        out.append(("fwd", k))
        if k + DEPTH < n:
            out.append(("weight", k + DEPTH))
        out.append(("own", k))
        if k >= 1:
            out.append(("epi", k - 1))
        if k >= 2:
            out.append(("bwd", k - 2))
    out += [("epi", n - 1), ("own_dx", 0)]
    if n >= 2:
        out.append(("bwd", n - 2))
    out += [("far_part", 0), ("own_sum", 0), ("far_dx", 0), ("bwd", n - 1), ("far_sum", 0)]
    out += [("own_home", 0), ("dot", 0)]
    out += [("finish", k) for k in range(n - 2)]
    out.append(("far_home", 0))
    out += [("finish", k) for k in range(max(n - 2, 0), n)]
    out.append(("input", 0))
    return out


def per_device(tokens, norm_gain, coded, block_codes, grid, cotangent):
    n_dev = lax.axis_size("narrow")
    n_wide = lax.axis_size("wide")
    n_a = 2
    n_b = n_dev // (2 * n_a)
    me = lax.axis_index("narrow")
    core, a, b = me % 2, me // 2 % n_a, me // (2 * n_a)
    w = lax.axis_index("wide")
    rows, fcols = coded.shape
    half = fcols // 2
    ntok, d_model = tokens.shape

    def move(x, to):
        pairs = []
        for n in range(n_dev):
            c0, a0, b0 = n % 2, n // 2 % n_a, n // (2 * n_a)
            b1, a1, c1 = to(b0, a0, c0)
            pairs.append((n, (b1 % n_b * n_a + a1 % n_a) * 2 + c1 % 2))
        return lax.ppermute(x, "narrow", pairs)

    def move_wide(x, pairs):
        return lax.ppermute(x, "wide", pairs)

    def move_all(x, to):
        pairs = []
        for w0 in range(n_wide):
            for i in range(n_dev):
                goal = to(w0 // n_a, w0 % n_a, i // (2 * n_a), i // 2 % n_a, i % 2)
                if goal is not None:
                    bw1, aw1, b1, a1, c1 = goal
                    at = (bw1 * n_a + aw1) * n_dev + (b1 * n_a + a1) * 2 + c1
                    pairs.append((w0 * n_dev + i, at))
        return lax.ppermute(x, ("wide", "narrow"), pairs)

    def to_core(x):
        return move(x, lambda b0, a0, c0: (b0, a0, c0 + 1))

    def to_a(x):
        return move(x, lambda b0, a0, c0: (b0, a0 + 1, c0))

    def to_b(x, step, cross):
        return move(x, lambda b0, a0, c0: (b0 + step, a0, c0 + cross))

    onehot = (
        block_codes[:, :, None] == jnp.arange(grid.shape[0], dtype=jnp.int32)[None, None, :]
    ).astype(jnp.float32)
    scale = jnp.sum(onehot * grid[None, None, :], axis=-1) / jnp.sqrt(jnp.float32(BLOCK))
    hblk = half // BLOCK

    def my_half(x, c, width):
        return lax.dynamic_slice_in_dim(x, c * width, width, 1)

    coded_c = [my_half(coded, core, half), my_half(coded, 1 - core, half)]
    scale_c = [my_half(scale, core, hblk), my_half(scale, 1 - core, hblk)]
    parts = cuts(hblk, CHUNKS)


    last = [coded]

    def after(*xs):
        return lax.optimization_barrier((*xs, last[0]))[: len(xs)]

    def mark(x):
        last[0] = x
        return x

    weights = [None] * len(parts)

    def columns_for(x, a_to, c_to):
        out = []
        for s in range(n_b):
            for q in range(2):
                at = (((b + s) % n_b) * n_a + a_to) * 2 + (c_to + q) % 2
                out.append(lax.dynamic_slice_in_dim(x, at * rows, rows, 1))
        return jnp.concatenate(out, axis=1)

    def flip(x):
        out = []
        for s in range(n_b):
            at = 2 * s * rows
            out += [x[:, at + rows : at + 2 * rows], x[:, at : at + rows]]
        return jnp.concatenate(out, axis=1)

    def norm(x):
        x = x.astype(jnp.float32)
        inv = lax.rsqrt(jnp.mean(x * x, axis=-1, keepdims=True) + 1e-05)
        return (x * inv * norm_gain[None, :]).astype(jnp.bfloat16), inv

    part_rows = ntok // n_wide
    v = {}
    v["x"] = jnp.zeros((4 * ntok, 2 * n_b * rows), jnp.bfloat16)
    v["act"] = jnp.zeros((ntok, fcols), jnp.bfloat16)
    v["dw"] = jnp.zeros((rows, fcols), jnp.float32)
    v["dot"] = jnp.zeros((2 * ntok,), jnp.float32)
    state = [dict() for _ in parts]
    mine_at, other_at = core * half, (1 - core) * half
    b_w, a_w = w // n_a, w % n_a

    def put(x, at):
        v["x"] = lax.dynamic_update_slice(v["x"], x, (at, 0))

    def share(_):
        part = lax.dynamic_slice_in_dim(tokens, w * part_rows, part_rows, 0)
        part, _ = norm(part)
        v["share"] = to_a(mark(columns_for(part, (a + 1) % n_a, core)))

    def weight(k):
        lo, hi = parts[k]
        mine, other = after(*[coded_c[i][:, lo:hi] for i in (0, 1)])
        mine, other = [
            decode(x, scale_c[i][:, lo // BLOCK : hi // BLOCK]) for i, x in enumerate((mine, other))
        ]
        mark(other)
        mark(mine)
        got = [mine, None]
        for step in range(1, n_b):
            got.append(to_b(mine, -step, 0))
            got.append(to_b(other, -step, 1))
        got[1] = to_core(other)
        weights[k] = got

    def norm_all(_):
        (held,) = after(tokens)
        v["normed"], v["inv"] = norm(held)
        mark(v["normed"])

    def cot_swap(_):
        (held,) = after(cotangent)
        got = to_core(mark(my_half(held, 1 - core, half)))
        v["cot"] = (my_half(held, core, half), got)

    def near(_):
        (held,) = after(v["normed"])
        other = mark(columns_for(held, a, 1 - core))
        v["near"] = to_core(other)
        (v["own"],) = after(columns_for(held, a, core))

    def far(_):
        (got,) = after(v["share"])
        put(got, 2 * ntok + w * part_rows)
        mark(got)
        v["far"] = [
            (step, move_wide(got, [(i, i ^ step) for i in range(n_wide)]))
            for step in range(1, n_wide)
        ]

    def cross(_):
        got = after(*[x for _, x in v["far"]])
        for (step, _), x in zip(v["far"], got):
            put(x, 2 * ntok + (w ^ step) * part_rows)
        got = to_core(mark(flip(v["x"][2 * ntok : 3 * ntok])))
        put(v["own"], 0)
        put(v["near"], ntok)
        put(got, 3 * ntok)

    def fwd(k):
        st = state[k]
        got = after(*weights[k])
        st["w"] = jnp.concatenate(got, axis=0)
        far_pre = jnp.dot(v["x"][2 * ntok :], st["w"], preferred_element_type=jnp.float32)
        far_pre = mark(far_pre.astype(jnp.bfloat16))
        st["far_pre"] = to_a(far_pre)

    def own(k):
        st = state[k]
        (wk,) = after(st["w"])
        st["pre"] = mark(jnp.dot(v["x"][: 2 * ntok], wk, preferred_element_type=jnp.float32))

    def epi(k):
        st, (lo, hi) = state[k], parts[k]
        far_pre, pre = after(st["far_pre"], st["pre"])
        cot = jnp.concatenate([x[:, lo:hi] for x in v["cot"]], axis=0).astype(jnp.float32)
        pre = pre + far_pre.astype(jnp.float32)
        sig = jax.nn.sigmoid(pre)
        act = (pre * sig).astype(jnp.bfloat16)
        grad = (cot * sig * (1.0 + pre * (1.0 - sig))).astype(jnp.bfloat16)
        v["dot"] = v["dot"] + jnp.sum(grad.astype(jnp.float32) * pre, axis=1)
        st["grad"], st["grad_far"] = mark(grad), to_a(grad)
        v["act"] = lax.dynamic_update_slice(v["act"], act[:ntok], (0, mine_at + lo))
        st["act"] = to_core(act[ntok:])

    def both(k):
        st = state[k]
        if "both" not in st:
            st["both"] = jnp.concatenate(after(st["grad"], st["grad_far"]), axis=0)
        return st["both"]

    def bwd(k):
        st = state[k]
        (grad,) = after(both(k))
        dw = lax.dot_general(
            v["x"], grad, (((0,), (0,)), ((), ())), preferred_element_type=jnp.float32
        )
        piece = [dw[i * rows : (i + 1) * rows] for i in range(2 * n_b)]
        low = [p.astype(jnp.bfloat16) for p in piece[1:]]
        mark(low[-1])
        st["mine"], st["other"] = [piece[0]], []
        for step in range(1, n_b):
            st["mine"].append(to_b(low[2 * step - 1], step, 0))
            st["other"].append(to_b(low[2 * step], step, 1))
        st["other"].append(to_core(low[0]))

    def across(grads, ws):
        return lax.dot_general(
            jnp.concatenate(grads, axis=1), jnp.concatenate(ws, axis=1),
            (((1,), (1,)), ((), ())), preferred_element_type=jnp.float32,
        )

    def core_swap(block):
        low = mark(block[ntok:].astype(jnp.bfloat16))
        got = [to_core(low[:, (i ^ 1) * rows : ((i ^ 1) + 1) * rows]) for i in range(2 * n_b)]
        return block[:ntok], got

    def own_dx(_):
        grads = after(*[st["grad"] for st in state])
        v["own_dx"] = core_swap(across(grads, [st["w"] for st in state]))

    def far_part(_):
        if len(parts) > 1:
            grads = after(*[st["grad_far"] for st in state[:-1]])
            v["far_part"] = mark(across(grads, [st["w"] for st in state[:-1]]))

    def far_dx(_):
        (grad,) = after(state[-1]["grad_far"])
        block = across([grad], [state[-1]["w"]])
        if len(parts) > 1:
            block = block + v["far_part"]
        v["far_dx"] = core_swap(block)

    def wide_sum(block, got):
        got = after(*got)
        total = jnp.concatenate(
            [block[:, i * rows : (i + 1) * rows] + x.astype(jnp.float32) for i, x in enumerate(got)],
            axis=1,
        )
        low = mark(total.astype(jnp.bfloat16))

        def home_block(x, step):
            at = (b_w + step - b) % n_b * 2 * rows
            return lax.dynamic_slice_in_dim(x, at, 2 * rows, 1)

        part = [home_block(low, 0)]
        for step in range(1, n_b):
            pairs = [(i, (i // n_a + step) % n_b * n_a + i % n_a) for i in range(n_wide)]
            part.append(move_wide(home_block(low, step), pairs))
        return part

    def own_sum(_):
        v["own_dx"] = wide_sum(*v["own_dx"])

    def far_sum(_):
        v["far_dx"] = wide_sum(*v["far_dx"])

    def own_home(_):
        got = after(*v["own_dx"])
        v["own_part"] = mark(sum(x.astype(jnp.float32) for x in got).astype(jnp.bfloat16))
        v["own_got"] = move_all(
            v["own_part"], lambda bw, aw, b0, a0, c0: (bw, a0, b0, a0, c0) if aw != a0 else None
        )

    def far_home(_):
        got = after(*v["far_dx"])
        part = mark(sum(x.astype(jnp.float32) for x in got).astype(jnp.bfloat16))
        v["far_got"] = [
            move_all(
                part,
                lambda bw, aw, b0, a0, c0: (bw, a0, b0, 1 - a0, c0) if (aw == a0) == same else None,
            )
            for same in (True, False)
        ]

    def dot(_):
        (total,) = after(v["dot"])
        total = total[:ntok] + to_core(total[ntok:])
        step = 1
        while step < n_wide:
            total = total + move_wide(total, [(i, i ^ step) for i in range(n_wide)])
            step *= 2
        v["row_dot"] = mark(total[:, None] / (v["inv"] * d_model))

    def finish(k):
        st, (lo, hi) = state[k], parts[k]
        got = after(st["act"], *st["mine"], *st["other"])
        act, mine, other = got[0], got[1 : 1 + n_b], got[1 + n_b :]
        v["act"] = lax.dynamic_update_slice(v["act"], act, (0, other_at + lo))
        mine = sum(x.astype(jnp.float32) for x in mine)
        other = sum(x.astype(jnp.float32) for x in other)
        v["dw"] = lax.dynamic_update_slice(v["dw"], mine, (0, mine_at + lo))
        v["dw"] = lax.dynamic_update_slice(v["dw"], other, (0, other_at + lo))
        mark(mine)

    def input_grad(_):
        own_part, own_got, *far_got = after(v["own_part"], v["own_got"], *v["far_got"])
        got = jnp.where(
            a_w == a,
            own_part.astype(jnp.float32) + own_got.astype(jnp.float32),
            sum(x.astype(jnp.float32) for x in far_got),
        )
        first, second = got[:, :rows], got[:, rows:]
        normed_grad = jnp.concatenate(
            [jnp.where(core == 0, first, second), jnp.where(core == 0, second, first)], axis=1
        )
        width = d_model // n_wide
        block = lax.dynamic_slice_in_dim(tokens, w * width, width, 1).astype(jnp.float32)
        gain = lax.dynamic_slice_in_dim(norm_gain, w * width, width, 0)
        inv = v["inv"]
        v["out"] = mark(
            (inv * (normed_grad * gain[None, :]) - block * inv**3 * v["row_dot"]).astype(jnp.bfloat16)
        )

    run = {
        "share": share, "weight": weight, "norm": norm_all, "cot": cot_swap, "near": near,
        "far": far, "cross": cross, "fwd": fwd, "own": own, "epi": epi, "bwd": bwd,
        "own_dx": own_dx, "far_part": far_part, "own_sum": own_sum, "far_dx": far_dx,
        "far_sum": far_sum, "own_home": own_home, "far_home": far_home, "dot": dot,
        "finish": finish, "input": input_grad,
    }
    for name, k in plan(len(parts)):
        run[name](k)
    return (v["act"], v["dw"], v["out"])


def solution(mesh):
    placed = (
        P("narrow", None),
        P(),
        P("narrow", "wide"),
        P("narrow", "wide"),
        P(),
        P("narrow", "wide"),
    )

    return jax.shard_map(
        per_device,
        mesh=mesh,
        in_specs=placed,
        out_specs=(P("narrow", "wide"), P("narrow", "wide"), P("narrow", "wide")),
        check_vma=False,
    )
```
